128 devices in a mesh: lat: 16 (over z, x), lon: 4 (over y), lev: 2 (over core).
Axes of the slice: x: 4, y: 4, z: 4, core: 2. Of those that a mesh axis runs over, the one named last changes fastest.
Arguments:
- initial_heat: float32 [256, 32, 192, 128], P('lat', 'lon', 'lev'), may hold values from 0.2 to 1.8
- scaled_wind_north: float32 [256, 32, 192, 128], P('lat', 'lon', 'lev'), may hold values from -0.3 to 0.3
- scaled_wind_east: float32 [256, 32, 192, 128], P('lat', 'lon', 'lev'), may hold values from -0.3 to 0.3
- scaled_wind_vertical: float32 [256, 32, 192, 128], P('lat', 'lon', 'lev'), may hold values from -0.3 to 0.3
Outputs:
- accumulated_eastward: float32 [256, 32, 192, 128], P('lat', 'lon', 'lev')
- temperature_end: float32 [256, 32, 192, 128], P('lat', 'lon', 'lev')
The draws below stay inside these ranges and needn't reach their ends.
All inputs are finite; a program needn't handle non-finite values.
Results may differ from the reference program's by a relative error of at most 0.00002.
Values sent between devices are 32-bit elements; how exact they have to be, the bound alone decides.
A program may use at most 448 MiB of HBM per device.

```python
import jax
import jax.numpy as jnp
from jax import lax

NORTHWARD_BOXES = 256
EASTWARD_BOXES = 32
UPWARD_BOXES = 192
LAYER_TOTAL = 128
STEPS = 6


def levels(own_key, shape, pieces, least, high):
    def one(dim, blocks):
        draws = jax.random.uniform(jax.random.fold_in(jax.random.fold_in(own_key, 6), dim), (blocks,), jnp.float32, least / len(pieces), high / len(pieces))
        return jnp.repeat(jnp.exp(draws), shape[dim] // blocks).reshape((-1,) + (1,) * (len(shape) - dim - 1))

    factor_of = one(*pieces[0])
    for cut in pieces[1:]:
        factor_of = factor_of * one(*cut)
    return factor_of


def setup_inputs(seed: int = 0) -> dict:
    key_list = jax.random.split(jax.random.key(seed), 5)
    return {
        "initial_heat": jnp.clip(0.2 + 1.5999999 * jax.random.uniform(key_list[0], (NORTHWARD_BOXES, EASTWARD_BOXES, UPWARD_BOXES, LAYER_TOTAL), jnp.float32) ** levels(key_list[0], (NORTHWARD_BOXES, EASTWARD_BOXES, UPWARD_BOXES, LAYER_TOTAL), ((0, 16), (1, 4), (2, 2)), -0.2, 0.2), 0.2, 1.8),
        "scaled_wind_north": jnp.clip(jax.random.uniform(key_list[1], (NORTHWARD_BOXES, EASTWARD_BOXES, UPWARD_BOXES, LAYER_TOTAL), jnp.float32, -0.3, 0.3) * levels(key_list[1], (NORTHWARD_BOXES, EASTWARD_BOXES, UPWARD_BOXES, LAYER_TOTAL), ((0, 16), (1, 4), (2, 2)), -0.4, 0.0), -0.3, 0.3),
        "scaled_wind_east": jnp.clip(jax.random.uniform(key_list[2], (NORTHWARD_BOXES, EASTWARD_BOXES, UPWARD_BOXES, LAYER_TOTAL), jnp.float32, -0.3, 0.3) * levels(key_list[2], (NORTHWARD_BOXES, EASTWARD_BOXES, UPWARD_BOXES, LAYER_TOTAL), ((0, 16), (1, 4), (2, 2)), -0.4, 0.0), -0.3, 0.3),
        "scaled_wind_vertical": jnp.clip(jax.random.uniform(key_list[3], (NORTHWARD_BOXES, EASTWARD_BOXES, UPWARD_BOXES, LAYER_TOTAL), jnp.float32, -0.3, 0.3) * levels(key_list[3], (NORTHWARD_BOXES, EASTWARD_BOXES, UPWARD_BOXES, LAYER_TOTAL), ((0, 16), (1, 4), (2, 2)), -0.4, 0.0), -0.3, 0.3),
    }


def strip_edges(values, dims):
    for dim in dims:
        values = lax.slice_in_dim(values, 1, values.shape[dim] - 1, axis=dim)
    return values


def neighbour(values, dim, start, dims):
    others = [other for other in dims if other != dim]
    values = strip_edges(values, others)
    return lax.slice_in_dim(values, start, start + values.shape[dim] - 2, axis=dim)


def single_update(extended_field, scaled_wind_north, scaled_wind_east, scaled_wind_vertical):
    middle = strip_edges(extended_field, (0, 1, 2))
    lower = [neighbour(extended_field, dim, 0, (0, 1, 2)) for dim in (0, 1, 2)]
    upper = [neighbour(extended_field, dim, 2, (0, 1, 2)) for dim in (0, 1, 2)]
    slopes = [above - beneath_layer for above, beneath_layer in zip(upper, lower)]
    smooth_rate = 0.05
    spread = lower[0] + upper[0] + lower[1] + upper[1] + lower[2] + upper[2] - 6.0 * middle
    return middle - scaled_wind_north * slopes[0] - scaled_wind_east * slopes[1] - scaled_wind_vertical * slopes[2] + smooth_rate * spread


def reference(initial_heat, scaled_wind_north, scaled_wind_east, scaled_wind_vertical):
    for step in range(STEPS):
        initial_heat = single_update(jnp.pad(initial_heat, ((1, 1), (1, 1), (1, 1), (0, 0)), mode="constant"), scaled_wind_north, scaled_wind_east, scaled_wind_vertical)
    accumulated_eastward = jnp.cumsum(initial_heat, axis=1) / EASTWARD_BOXES
    return accumulated_eastward, initial_heat
```

```python
import functools

import jax
import jax.numpy as jnp
from jax import lax
from jax.experimental import pallas as pl
from jax.experimental.pallas import tpu as pltpu
from jax.sharding import PartitionSpec as P

STEPS = 6
PAD = 8
MESH = pl.DeviceIdType.MESH


def row_at(k, rows):
    odd = k % 2
    return (1 - odd) * (k // 2) + odd * (rows - 1 - k // 2)


def kernel(
    sizes,
    heat,
    north,
    east,
    up,
    acc,
    end,
    field,
    wind,
    carry,
    onward,
    edge_out,
    edge_in,
    load_sem,
    lon_send,
    lon_recv,
    lat_send,
    lat_recv,
    lev_send,
    lev_recv,
    carry_send,
    carry_recv,
):
    lats, lons, levs = sizes
    rows, cols, deep, members = heat.shape
    lat, lon, lev = (lax.axis_index(name) for name in ("lat", "lon", "lev"))
    body = pl.ds(PAD, deep)

    def remote(src, dst, send, recv, axis, to):
        return pltpu.make_async_remote_copy(
            src_ref=src,
            dst_ref=dst,
            send_sem=send,
            recv_sem=recv,
            device_id={axis: to},
            device_id_type=MESH,
        )

    def lon_copy(slot, y, side, src=None):
        x = (0, cols - 1)[side]
        src = field.at[slot, y + 1, x + 1, body] if src is None else src.at[y, x]
        dst = field.at[slot, y + 1, (cols + 1, 0)[side], body]
        to = lon + (-1, 1)[side]
        return remote(
            src, dst, lon_send.at[side, slot, y], lon_recv.at[side, slot, y], "lon", to
        )

    def lat_copy(slot, side, src=None):
        y = (0, rows - 1)[side]
        src = field.at[slot, y + 1, pl.ds(1, cols), body] if src is None else src.at[y]
        dst = field.at[slot, (rows + 1, 0)[side], pl.ds(1, cols), body]
        to = lat + (-1, 1)[side]
        return remote(
            src, dst, lat_send.at[side, slot], lat_recv.at[side, slot], "lat", to
        )

    def lev_copy(slot, y):
        return remote(
            edge_out.at[slot, y],
            edge_in.at[slot, y],
            lev_send.at[slot, y],
            lev_recv.at[slot, y],
            "lev",
            1 - lev,
        )

    def carry_copy(y):
        return remote(
            onward.at[y], carry.at[y], carry_send.at[y], carry_recv.at[y], "lon", lon + 1
        )

    lon_has = (lon > 0, lon < lons - 1)
    lat_has = (lat > 0, lat < lats - 1)

    def load_heat(y):
        return pltpu.make_async_copy(
            heat.at[y], field.at[0, y + 1, pl.ds(1, cols), body], load_sem.at[3, y]
        )

    def load_wind(d, y):
        return pltpu.make_async_copy(
            (north, east, up)[d].at[y], wind.at[d, y], load_sem.at[d, y]
        )

    barrier = pltpu.get_barrier_semaphore()

    def greet(axis, to):
        pl.semaphore_signal(
            barrier, inc=1, device_id={axis: to}, device_id_type=MESH
        )

    for side in (0, 1):
        pl.when(lon_has[side])(lambda: greet("lon", lon + (-1, 1)[side]))
        pl.when(lat_has[side])(lambda: greet("lat", lat + (-1, 1)[side]))
    greet("lev", 1 - lev)

    def start_heat(k, _):
        load_heat(row_at(k, rows)).start()
        return 0

    def start_wind(k, _):
        for d in range(3):
            load_wind(d, row_at(k, rows)).start()
        return 0

    lax.fori_loop(0, rows, start_heat, 0)
    lax.fori_loop(0, rows, start_wind, 0)

    peers = 1 + sum(has.astype(jnp.int32) for has in (*lon_has, *lat_has))
    pl.semaphore_wait(barrier, peers)

    for side in (0, 1):
        pl.when(lat_has[side])(lambda: lat_copy(0, side, heat).start())

    def start_lon(k, _):
        y = row_at(k, rows)
        for side in (0, 1):
            pl.when(lon_has[side])(lambda: lon_copy(0, y, side, heat).start())
        return 0

    lax.fori_loop(0, rows, start_lon, 0)

    def clear_row(y, _):
        for slot in (0, 1):
            field[slot, y + 1, pl.ds(1, cols), pl.ds(0, PAD), :] = jnp.zeros(
                (cols, PAD, members), jnp.float32
            )
            field[slot, y + 1, pl.ds(1, cols), pl.ds(PAD + deep, PAD), :] = jnp.zeros(
                (cols, PAD, members), jnp.float32
            )
            for side in (0, 1):

                @pl.when(jnp.logical_not(lon_has[side]))
                def _():
                    field[slot, y + 1, (0, cols + 1)[side], body, :] = jnp.zeros(
                        (deep, members), jnp.float32
                    )

        return 0

    lax.fori_loop(0, rows, clear_row, 0)

    def clear_lat(x, _):
        for slot in (0, 1):
            for side in (0, 1):

                @pl.when(jnp.logical_not(lat_has[side]))
                def _():
                    field[slot, (0, rows + 1)[side], x + 1, body, :] = jnp.zeros(
                        (deep, members), jnp.float32
                    )

        return 0

    lax.fori_loop(0, cols, clear_lat, 0)

    edge_from = PAD + (1 - lev) * (deep - 1)
    edge_to = PAD - 1 + (1 - lev) * (deep + 1)

    def first_edges(k, _):
        y = row_at(k, rows)
        load_heat(y).wait()

        def one(x, _):
            edge_out[0, y, pl.ds(x, 1), :] = field[
                0, y + 1, x + 1, pl.ds(edge_from, 1), :
            ]
            return 0

        lax.fori_loop(0, cols, one, 0)
        lev_copy(0, y).start()
        return 0

    lax.fori_loop(0, rows, first_edges, 0)

    def updated(slot, y, x):
        field[slot, y + 1, x + 1, pl.ds(edge_to, 1), :] = edge_in[
            slot, y, pl.ds(x, 1), :
        ]
        middle = field[slot, y + 1, x + 1, body, :]
        lower = (
            field[slot, y, x + 1, body, :],
            field[slot, y + 1, x, body, :],
            field[slot, y + 1, x + 1, pl.ds(PAD - 1, deep), :],
        )
        upper = (
            field[slot, y + 2, x + 1, body, :],
            field[slot, y + 1, x + 2, body, :],
            field[slot, y + 1, x + 1, pl.ds(PAD + 1, deep), :],
        )
        spread = (
            lower[0] + upper[0] + lower[1] + upper[1] + lower[2] + upper[2]
        ) - 6.0 * middle
        value = middle + 0.05 * spread
        for d in range(3):
            value = value - wind[d, y, x, :, :] * (upper[d] - lower[d])
        return value

    def arrivals(slot, y):
        for side in (0, 1):
            pl.when(lon_has[side])(lambda: lon_copy(slot, y, 1 - side).wait_recv())
            pl.when(jnp.logical_and(lat_has[side], y == (0, rows - 1)[side]))(
                lambda: lat_copy(slot, 1 - side).wait_recv()
            )
        lev_copy(slot, y).wait_recv()

    def departures(slot, y):
        for side in (0, 1):
            pl.when(lon_has[side])(lambda: lon_copy(slot, y, side).wait_send())
            pl.when(jnp.logical_and(lat_has[side], y == (0, rows - 1)[side]))(
                lambda: lat_copy(slot, side).wait_send()
            )
        lev_copy(slot, y).wait_send()

    def step(t, _):
        now = t % 2
        later = 1 - now

        def one_row(k, _):
            y = row_at(k, rows)

            @pl.when(t == 0)
            def _():
                for d in range(3):
                    load_wind(d, y).wait()

            arrivals(now, y)
            pl.when(t > 0)(lambda: departures(later, y))

            def one(x, _):
                field[later, y + 1, x + 1, body, :] = updated(now, y, x)
                edge_out[later, y, pl.ds(x, 1), :] = field[
                    later, y + 1, x + 1, pl.ds(edge_from, 1), :
                ]
                return 0

            lax.fori_loop(0, cols, one, 0)
            for side in (0, 1):
                pl.when(lon_has[side])(lambda: lon_copy(later, y, side).start())
                pl.when(jnp.logical_and(lat_has[side], y == (0, rows - 1)[side]))(
                    lambda: lat_copy(later, side).start()
                )
            lev_copy(later, y).start()
            return 0

        lax.fori_loop(0, rows, one_row, 0)
        return 0

    lax.fori_loop(0, STEPS - 1, step, 0)

    last = (STEPS - 1) % 2

    def last_row(k, _):
        y = row_at(k, rows)
        arrivals(last, y)
        departures(1 - last, y)

        def one(x, total):
            value = updated(last, y, x)
            end[y, x, :, :] = value
            total = total + value
            acc[y, x, :, :] = total
            return total

        total = lax.fori_loop(
            0, cols, one, jnp.zeros((deep, members), jnp.float32)
        )

        @pl.when(lon == 0)
        def _():
            onward[y, :, :] = total
            carry_copy(y).start()

        departures(last, y)
        return 0

    lax.fori_loop(0, rows, last_row, 0)

    scale = 1.0 / (cols * lons)

    def finish(k, _):
        y = row_at(k, rows)

        @pl.when(lon > 0)
        def _():
            carry_copy(y).wait_recv()

            @pl.when(lon < lons - 1)
            def _():
                onward[y, :, :] = carry[y, :, :] + acc[y, cols - 1, :, :]
                carry_copy(y).start()

        @pl.when(lon == 0)
        def _():
            carry[y, :, :] = jnp.zeros((deep, members), jnp.float32)

        before = carry[y, :, :]

        def one(x, _):
            acc[y, x, :, :] = (acc[y, x, :, :] + before) * scale
            return 0

        lax.fori_loop(0, cols, one, 0)
        return 0

    lax.fori_loop(0, rows, finish, 0)

    @pl.when(lon < lons - 1)
    def _():
        def drain(k, _):
            carry_copy(row_at(k, rows)).wait_send()
            return 0

        lax.fori_loop(0, rows, drain, 0)


def per_device(sizes, heat, north, east, up):
    rows, cols, deep, members = heat.shape
    shape = jax.ShapeDtypeStruct(heat.shape, heat.dtype)
    f32 = jnp.float32
    dma = pltpu.SemaphoreType.DMA
    return pl.pallas_call(
        functools.partial(kernel, sizes),
        out_shape=(shape, shape),
        in_specs=[pl.BlockSpec(memory_space=pl.ANY)] * 4,
        out_specs=(pl.BlockSpec(memory_space=pltpu.VMEM),) * 2,
        scratch_shapes=[
            pltpu.VMEM((2, rows + 2, cols + 2, deep + 2 * PAD, members), f32),
            pltpu.VMEM((3, rows, cols, deep, members), f32),
            pltpu.VMEM((rows, deep, members), f32),
            pltpu.VMEM((rows, deep, members), f32),
            pltpu.VMEM((2, rows, cols, members), f32),
            pltpu.VMEM((2, rows, cols, members), f32),
            dma((4, rows)),
            dma((2, 2, rows)),
            dma((2, 2, rows)),
            dma((2, 2)),
            dma((2, 2)),
            dma((2, rows)),
            dma((2, rows)),
            dma((rows,)),
            dma((rows,)),
        ],
        compiler_params=pltpu.CompilerParams(
            collective_id=0,
            has_side_effects=True,
            vmem_limit_bytes=40 * 1024 * 1024,
        ),
    )(heat, north, east, up)


def solution(mesh):
    sizes = tuple(mesh.shape[name] for name in ("lat", "lon", "lev"))
    spec = P("lat", "lon", "lev", None)
    return jax.shard_map(
        functools.partial(per_device, sizes),
        mesh=mesh,
        in_specs=(spec,) * 4,
        out_specs=(spec, spec),
        check_vma=False,
    )
```

```python
import functools

import jax
import jax.numpy as jnp
from jax import lax
from jax.experimental import pallas as pl
from jax.experimental.pallas import tpu as pltpu
from jax.sharding import PartitionSpec as P

STEPS = 6
PAD = 8
MESH = pl.DeviceIdType.MESH


def row_at(k, rows):
    odd = k % 2
    return (1 - odd) * (k // 2) + odd * (rows - 1 - k // 2)


def kernel(
    sizes,
    heat,
    north,
    east,
    up,
    acc,
    end,
    field,
    wind,
    carry,
    onward,
    edge_out,
    edge_in,
    load_sem,
    lon_send,
    lon_recv,
    lat_send,
    lat_recv,
    lev_send,
    lev_recv,
    carry_send,
    carry_recv,
):
    lats, lons, levs = sizes
    rows, cols, deep, members = heat.shape
    lat, lon, lev = (lax.axis_index(name) for name in ("lat", "lon", "lev"))
    body = pl.ds(PAD, deep)

    def remote(src, dst, send, recv, axis, to):
        return pltpu.make_async_remote_copy(
            src_ref=src,
            dst_ref=dst,
            send_sem=send,
            recv_sem=recv,
            device_id={axis: to},
            device_id_type=MESH,
        )

    def lon_copy(slot, y, side, src=None):
        x = (0, cols - 1)[side]
        src = field.at[slot, y + 1, x + 1, body] if src is None else src.at[y, x]
        dst = field.at[slot, y + 1, (cols + 1, 0)[side], body]
        to = lon + (-1, 1)[side]
        return remote(
            src, dst, lon_send.at[side, slot, y], lon_recv.at[side, slot, y], "lon", to
        )

    def lat_copy(slot, side, src=None):
        y = (0, rows - 1)[side]
        src = field.at[slot, y + 1, pl.ds(1, cols), body] if src is None else src.at[y]
        dst = field.at[slot, (rows + 1, 0)[side], pl.ds(1, cols), body]
        to = lat + (-1, 1)[side]
        return remote(
            src, dst, lat_send.at[side, slot], lat_recv.at[side, slot], "lat", to
        )

    def lev_copy(slot, y):
        return remote(
            edge_out.at[slot, y],
            edge_in.at[slot, y],
            lev_send.at[slot, y],
            lev_recv.at[slot, y],
            "lev",
            1 - lev,
        )

    def carry_copy(y):
        return remote(
            onward.at[y], carry.at[y], carry_send.at[y], carry_recv.at[y], "lon", lon + 1
        )

    lon_has = (lon > 0, lon < lons - 1)
    lat_has = (lat > 0, lat < lats - 1)

    def load_heat(y):
        return pltpu.make_async_copy(
            heat.at[y], field.at[0, y + 1, pl.ds(1, cols), body], load_sem.at[3, y]
        )

    def load_wind(d, y):
        return pltpu.make_async_copy(
            (north, east, up)[d].at[y], wind.at[d, y], load_sem.at[d, y]
        )

    barrier = pltpu.get_barrier_semaphore()

    def greet(axis, to):
        pl.semaphore_signal(
            barrier, inc=1, device_id={axis: to}, device_id_type=MESH
        )

    for side in (0, 1):
        pl.when(lon_has[side])(lambda: greet("lon", lon + (-1, 1)[side]))
        pl.when(lat_has[side])(lambda: greet("lat", lat + (-1, 1)[side]))
    greet("lev", 1 - lev)

    def start_heat(k, _):
        load_heat(row_at(k, rows)).start()
        return 0

    def start_wind(k, _):
        for d in range(3):
            load_wind(d, row_at(k, rows)).start()
        return 0

    lax.fori_loop(0, rows, start_heat, 0)
    lax.fori_loop(0, rows, start_wind, 0)

    peers = 1 + sum(has.astype(jnp.int32) for has in (*lon_has, *lat_has))
    pl.semaphore_wait(barrier, peers)

    for side in (0, 1):
        pl.when(lat_has[side])(lambda: lat_copy(0, side, heat).start())

    def start_lon(k, _):
        y = row_at(k, rows)
        for side in (0, 1):
            pl.when(lon_has[side])(lambda: lon_copy(0, y, side, heat).start())
        return 0

    lax.fori_loop(0, rows, start_lon, 0)

    def clear_row(y, _):
        for slot in (0, 1):
            field[slot, y + 1, pl.ds(1, cols), pl.ds(0, PAD), :] = jnp.zeros(
                (cols, PAD, members), jnp.float32
            )
            field[slot, y + 1, pl.ds(1, cols), pl.ds(PAD + deep, PAD), :] = jnp.zeros(
                (cols, PAD, members), jnp.float32
            )
            for side in (0, 1):

                @pl.when(jnp.logical_not(lon_has[side]))
                def _():
                    field[slot, y + 1, (0, cols + 1)[side], body, :] = jnp.zeros(
                        (deep, members), jnp.float32
                    )

        return 0

    lax.fori_loop(0, rows, clear_row, 0)

    def clear_lat(x, _):
        for slot in (0, 1):
            for side in (0, 1):

                @pl.when(jnp.logical_not(lat_has[side]))
                def _():
                    field[slot, (0, rows + 1)[side], x + 1, body, :] = jnp.zeros(
                        (deep, members), jnp.float32
                    )

        return 0

    lax.fori_loop(0, cols, clear_lat, 0)

    edge_from = PAD + (1 - lev) * (deep - 1)
    edge_to = PAD - 1 + (1 - lev) * (deep + 1)

    def first_edges(k, _):
        y = row_at(k, rows)
        load_heat(y).wait()

        def one(x, _):
            edge_out[0, y, pl.ds(x, 1), :] = field[
                0, y + 1, x + 1, pl.ds(edge_from, 1), :
            ]
            return 0

        lax.fori_loop(0, cols, one, 0)
        lev_copy(0, y).start()
        return 0

    lax.fori_loop(0, rows, first_edges, 0)

    def updated(slot, y, x):
        field[slot, y + 1, x + 1, pl.ds(edge_to, 1), :] = edge_in[
            slot, y, pl.ds(x, 1), :
        ]
        middle = field[slot, y + 1, x + 1, body, :]
        lower = (
            field[slot, y, x + 1, body, :],
            field[slot, y + 1, x, body, :],
            field[slot, y + 1, x + 1, pl.ds(PAD - 1, deep), :],
        )
        upper = (
            field[slot, y + 2, x + 1, body, :],
            field[slot, y + 1, x + 2, body, :],
            field[slot, y + 1, x + 1, pl.ds(PAD + 1, deep), :],
        )
        spread = (
            lower[0] + upper[0] + lower[1] + upper[1] + lower[2] + upper[2]
        ) - 6.0 * middle
        value = middle + 0.05 * spread
        for d in range(3):
            value = value - wind[d, y, x, :, :] * (upper[d] - lower[d])
        return value

    def arrivals(slot, y):
        for side in (0, 1):
            pl.when(lon_has[side])(lambda: lon_copy(slot, y, 1 - side).wait_recv())
            pl.when(jnp.logical_and(lat_has[side], y == (0, rows - 1)[side]))(
                lambda: lat_copy(slot, 1 - side).wait_recv()
            )
        lev_copy(slot, y).wait_recv()

    def departures(slot, y):
        for side in (0, 1):
            pl.when(lon_has[side])(lambda: lon_copy(slot, y, side).wait_send())
            pl.when(jnp.logical_and(lat_has[side], y == (0, rows - 1)[side]))(
                lambda: lat_copy(slot, side).wait_send()
            )
        lev_copy(slot, y).wait_send()

    def step(t, _):
        now = t % 2
        later = 1 - now

        def one_row(k, _):
            y = row_at(k, rows)

            @pl.when(t == 0)
            def _():
                for d in range(3):
                    load_wind(d, y).wait()

            arrivals(now, y)
            pl.when(t > 0)(lambda: departures(later, y))

            def one(x, _):
                field[later, y + 1, x + 1, body, :] = updated(now, y, x)
                edge_out[later, y, pl.ds(x, 1), :] = field[
                    later, y + 1, x + 1, pl.ds(edge_from, 1), :
                ]
                return 0

            lax.fori_loop(0, cols, one, 0)
            for side in (0, 1):
                pl.when(lon_has[side])(lambda: lon_copy(later, y, side).start())
                pl.when(jnp.logical_and(lat_has[side], y == (0, rows - 1)[side]))(
                    lambda: lat_copy(later, side).start()
                )
            lev_copy(later, y).start()
            return 0

        lax.fori_loop(0, rows, one_row, 0)
        return 0

    lax.fori_loop(0, STEPS - 1, step, 0)

    last = (STEPS - 1) % 2

    def last_row(k, _):
        y = row_at(k, rows)
        arrivals(last, y)
        departures(1 - last, y)

        def one(x, total):
            value = updated(last, y, x)
            end[y, x, :, :] = value
            total = total + value
            acc[y, x, :, :] = total
            return total

        total = lax.fori_loop(
            0, cols, one, jnp.zeros((deep, members), jnp.float32)
        )

        @pl.when(lon == 0)
        def _():
            onward[y, :, :] = total
            carry_copy(y).start()

        departures(last, y)
        return 0

    lax.fori_loop(0, rows, last_row, 0)

    scale = 1.0 / (cols * lons)

    def finish(k, _):
        y = row_at(k, rows)

        @pl.when(lon > 0)
        def _():
            carry_copy(y).wait_recv()

            @pl.when(lon < lons - 1)
            def _():
                onward[y, :, :] = carry[y, :, :] + acc[y, cols - 1, :, :]
                carry_copy(y).start()

        @pl.when(lon == 0)
        def _():
            carry[y, :, :] = jnp.zeros((deep, members), jnp.float32)

        before = carry[y, :, :]

        def one(x, _):
            acc[y, x, :, :] = (acc[y, x, :, :] + before) * scale
            return 0

        lax.fori_loop(0, cols, one, 0)
        return 0

    lax.fori_loop(0, rows, finish, 0)

    @pl.when(lon < lons - 1)
    def _():
        def drain(k, _):
            carry_copy(row_at(k, rows)).wait_send()
            return 0

        lax.fori_loop(0, rows, drain, 0)


def store_kernel(acc, end, acc_out, end_out, sem):
    def both(y):
        return (
            pltpu.make_async_copy(end.at[y], end_out.at[y], sem.at[0, y]),
            pltpu.make_async_copy(acc.at[y], acc_out.at[y], sem.at[1, y]),
        )

    for y in range(acc.shape[0]):
        for copy in both(y):
            copy.start()
    for y in range(acc.shape[0]):
        for copy in both(y):
            copy.wait()


def per_device(sizes, heat, north, east, up):
    rows, cols, deep, members = heat.shape
    shape = jax.ShapeDtypeStruct(heat.shape, heat.dtype)
    f32 = jnp.float32
    dma = pltpu.SemaphoreType.DMA
    acc, end = pl.pallas_call(
        functools.partial(kernel, sizes),
        out_shape=(shape, shape),
        in_specs=[pl.BlockSpec(memory_space=pl.ANY)] * 4,
        out_specs=(pl.BlockSpec(memory_space=pltpu.VMEM),) * 2,
        scratch_shapes=[
            pltpu.VMEM((2, rows + 2, cols + 2, deep + 2 * PAD, members), f32),
            pltpu.VMEM((3, rows, cols, deep, members), f32),
            pltpu.VMEM((rows, deep, members), f32),
            pltpu.VMEM((rows, deep, members), f32),
            pltpu.VMEM((2, rows, cols, members), f32),
            pltpu.VMEM((2, rows, cols, members), f32),
            dma((4, rows)),
            dma((2, 2, rows)),
            dma((2, 2, rows)),
            dma((2, 2)),
            dma((2, 2)),
            dma((2, rows)),
            dma((2, rows)),
            dma((rows,)),
            dma((rows,)),
        ],
        compiler_params=pltpu.CompilerParams(
            collective_id=0,
            has_side_effects=True,
            vmem_limit_bytes=40 * 1024 * 1024,
        ),
    )(heat, north, east, up)
    return pl.pallas_call(
        store_kernel,
        out_shape=(shape, shape),
        in_specs=[pl.BlockSpec(memory_space=pltpu.VMEM)] * 2,
        out_specs=(pl.BlockSpec(memory_space=pltpu.HBM),) * 2,
        scratch_shapes=[dma((2, rows))],
        compiler_params=pltpu.CompilerParams(vmem_limit_bytes=1024 * 1024),
    )(acc, end)


def solution(mesh):
    sizes = tuple(mesh.shape[name] for name in ("lat", "lon", "lev"))
    spec = P("lat", "lon", "lev", None)
    return jax.shard_map(
        functools.partial(per_device, sizes),
        mesh=mesh,
        in_specs=(spec,) * 4,
        out_specs=(spec, spec),
        check_vma=False,
    )
```

```python
import functools

import jax
import jax.numpy as jnp
from jax import lax
from jax.experimental import pallas as pl
from jax.experimental.pallas import tpu as pltpu
from jax.sharding import PartitionSpec as P

STEPS = 6
PAD = 8
MESH = pl.DeviceIdType.MESH


def row_at(k, rows):
    odd = k % 2
    return (1 - odd) * (k // 2) + odd * (rows - 1 - k // 2)


def kernel(
    sizes,
    heat,
    north,
    east,
    up,
    acc,
    end,
    field,
    wind,
    from_low,
    from_high,
    edge_out,
    edge_in,
    load_sem,
    lon_send,
    lon_recv,
    lat_send,
    lat_recv,
    lev_send,
    lev_recv,
    up_send,
    up_recv,
    down_send,
    down_recv,
):
    lats, lons, levs = sizes
    rows, cols, deep, members = heat.shape
    lat, lon, lev = (lax.axis_index(name) for name in ("lat", "lon", "lev"))
    body = pl.ds(PAD, deep)

    def remote(src, dst, send, recv, axis, to):
        return pltpu.make_async_remote_copy(
            src_ref=src,
            dst_ref=dst,
            send_sem=send,
            recv_sem=recv,
            device_id={axis: to},
            device_id_type=MESH,
        )

    def lon_copy(slot, y, side, src=None):
        x = (0, cols - 1)[side]
        src = field.at[slot, y + 1, x + 1, body] if src is None else src.at[y, x]
        dst = field.at[slot, y + 1, (cols + 1, 0)[side], body]
        to = lon + (-1, 1)[side]
        return remote(
            src, dst, lon_send.at[side, slot, y], lon_recv.at[side, slot, y], "lon", to
        )

    def lat_copy(slot, side, src=None):
        y = (0, rows - 1)[side]
        src = field.at[slot, y + 1, pl.ds(1, cols), body] if src is None else src.at[y]
        dst = field.at[slot, (rows + 1, 0)[side], pl.ds(1, cols), body]
        to = lat + (-1, 1)[side]
        return remote(
            src, dst, lat_send.at[side, slot], lat_recv.at[side, slot], "lat", to
        )

    def lev_copy(slot, y):
        return remote(
            edge_out.at[slot, y],
            edge_in.at[slot, y],
            lev_send.at[slot, y],
            lev_recv.at[slot, y],
            "lev",
            1 - lev,
        )

    def up_copy(y, src):
        return remote(
            src, from_low.at[y], up_send.at[y], up_recv.at[y], "lon", lon + 1
        )

    def down_copy(y, src):
        to = (lon + lons - 1) % lons
        return remote(
            src, from_high.at[y], down_send.at[y], down_recv.at[y], "lon", to
        )

    lon_has = (lon > 0, lon < lons - 1)
    lat_has = (lat > 0, lat < lats - 1)

    def load_heat(y):
        return pltpu.make_async_copy(
            heat.at[y], field.at[0, y + 1, pl.ds(1, cols), body], load_sem.at[3, y]
        )

    def load_wind(d, y):
        return pltpu.make_async_copy(
            (north, east, up)[d].at[y], wind.at[d, y], load_sem.at[d, y]
        )

    barrier = pltpu.get_barrier_semaphore()

    def greet(axis, to):
        pl.semaphore_signal(
            barrier, inc=1, device_id={axis: to}, device_id_type=MESH
        )

    for side in (0, 1):
        greet("lon", (lon + (lons - 1, 1)[side]) % lons)
        pl.when(lat_has[side])(lambda: greet("lat", lat + (-1, 1)[side]))
    greet("lev", 1 - lev)

    def start_heat(k, _):
        load_heat(row_at(k, rows)).start()
        return 0

    def start_wind(k, _):
        for d in range(3):
            load_wind(d, row_at(k, rows)).start()
        return 0

    lax.fori_loop(0, rows, start_heat, 0)
    lax.fori_loop(0, rows, start_wind, 0)

    peers = 3 + sum(has.astype(jnp.int32) for has in lat_has)
    pl.semaphore_wait(barrier, peers)

    for side in (0, 1):
        pl.when(lat_has[side])(lambda: lat_copy(0, side, heat).start())

    def start_lon(k, _):
        y = row_at(k, rows)
        for side in (0, 1):
            pl.when(lon_has[side])(lambda: lon_copy(0, y, side, heat).start())
        return 0

    lax.fori_loop(0, rows, start_lon, 0)

    def clear_row(y, _):
        for slot in (0, 1):
            field[slot, y + 1, pl.ds(1, cols), pl.ds(0, PAD), :] = jnp.zeros(
                (cols, PAD, members), jnp.float32
            )
            field[slot, y + 1, pl.ds(1, cols), pl.ds(PAD + deep, PAD), :] = jnp.zeros(
                (cols, PAD, members), jnp.float32
            )
            for side in (0, 1):

                @pl.when(jnp.logical_not(lon_has[side]))
                def _():
                    field[slot, y + 1, (0, cols + 1)[side], body, :] = jnp.zeros(
                        (deep, members), jnp.float32
                    )

        return 0

    lax.fori_loop(0, rows, clear_row, 0)

    def clear_lat(x, _):
        for slot in (0, 1):
            for side in (0, 1):

                @pl.when(jnp.logical_not(lat_has[side]))
                def _():
                    field[slot, (0, rows + 1)[side], x + 1, body, :] = jnp.zeros(
                        (deep, members), jnp.float32
                    )

        return 0

    lax.fori_loop(0, cols, clear_lat, 0)

    edge_from = PAD + (1 - lev) * (deep - 1)
    edge_to = PAD - 1 + (1 - lev) * (deep + 1)

    def first_edges(k, _):
        y = row_at(k, rows)
        load_heat(y).wait()

        def one(x, _):
            edge_out[0, y, pl.ds(x, 1), :] = field[
                0, y + 1, x + 1, pl.ds(edge_from, 1), :
            ]
            return 0

        lax.fori_loop(0, cols, one, 0)
        lev_copy(0, y).start()
        return 0

    lax.fori_loop(0, rows, first_edges, 0)

    def updated(slot, y, x):
        field[slot, y + 1, x + 1, pl.ds(edge_to, 1), :] = edge_in[
            slot, y, pl.ds(x, 1), :
        ]
        middle = field[slot, y + 1, x + 1, body, :]
        lower = (
            field[slot, y, x + 1, body, :],
            field[slot, y + 1, x, body, :],
            field[slot, y + 1, x + 1, pl.ds(PAD - 1, deep), :],
        )
        upper = (
            field[slot, y + 2, x + 1, body, :],
            field[slot, y + 1, x + 2, body, :],
            field[slot, y + 1, x + 1, pl.ds(PAD + 1, deep), :],
        )
        spread = (
            lower[0] + upper[0] + lower[1] + upper[1] + lower[2] + upper[2]
        ) - 6.0 * middle
        value = middle + 0.05 * spread
        for d in range(3):
            value = value - wind[d, y, x, :, :] * (upper[d] - lower[d])
        return value

    def arrivals(slot, y):
        for side in (0, 1):
            pl.when(lon_has[side])(lambda: lon_copy(slot, y, 1 - side).wait_recv())
            pl.when(jnp.logical_and(lat_has[side], y == (0, rows - 1)[side]))(
                lambda: lat_copy(slot, 1 - side).wait_recv()
            )
        lev_copy(slot, y).wait_recv()

    def departures(slot, y):
        for side in (0, 1):
            pl.when(lon_has[side])(lambda: lon_copy(slot, y, side).wait_send())
            pl.when(jnp.logical_and(lat_has[side], y == (0, rows - 1)[side]))(
                lambda: lat_copy(slot, side).wait_send()
            )
        lev_copy(slot, y).wait_send()

    def step(t, _):
        now = t % 2
        later = 1 - now

        def one_row(k, _):
            y = row_at(k, rows)

            @pl.when(t == 0)
            def _():
                for d in range(3):
                    load_wind(d, y).wait()

            arrivals(now, y)
            pl.when(t > 0)(lambda: departures(later, y))

            def one(x, _):
                field[later, y + 1, x + 1, body, :] = updated(now, y, x)
                edge_out[later, y, pl.ds(x, 1), :] = field[
                    later, y + 1, x + 1, pl.ds(edge_from, 1), :
                ]
                return 0

            lax.fori_loop(0, cols, one, 0)
            for side in (0, 1):
                pl.when(lon_has[side])(lambda: lon_copy(later, y, side).start())
                pl.when(jnp.logical_and(lat_has[side], y == (0, rows - 1)[side]))(
                    lambda: lat_copy(later, side).start()
                )
            lev_copy(later, y).start()
            return 0

        lax.fori_loop(0, rows, one_row, 0)
        return 0

    lax.fori_loop(0, STEPS - 1, step, 0)

    last = (STEPS - 1) % 2
    scale = 1.0 / (cols * lons)

    quarter = rows // 4

    def row_b(j):
        return row_at(4 * j, rows)

    def row_e(j):
        return row_at(4 * j + 1, rows)

    def row_a(j):
        return row_at(4 * j + 2, rows)

    def row_c(j):
        return row_at(4 * j + 3, rows)

    def own(y):
        return acc.at[y, cols - 1]

    def each(body_of):
        def one(j, _):
            body_of(j)
            return 0

        lax.fori_loop(0, quarter, one, 0)

    def last_row(k, _):
        y = row_at(k, rows)
        way = k % 4
        arrivals(last, y)
        departures(1 - last, y)

        def one(x, total):
            value = updated(last, y, x)
            end[y, x, :, :] = value
            total = total + value
            acc[y, x, :, :] = total * scale
            return total

        lax.fori_loop(0, cols, one, jnp.zeros((deep, members), jnp.float32))

        def first(place, number):
            return jnp.logical_and(lon == place, way == number)

        up_first = jnp.logical_or(
            first(0, 2), jnp.logical_or(first(1, 0), first(2, 3))
        )
        down_first = jnp.logical_or(
            first(0, 0), jnp.logical_or(first(1, 3), first(2, 1))
        )
        pl.when(up_first)(lambda: up_copy(y, own(y)).start())
        pl.when(down_first)(lambda: down_copy(y, own(y)).start())
        departures(last, y)
        return 0

    lax.fori_loop(0, rows, last_row, 0)

    def got_low(y):
        up_copy(y, own(y)).wait_recv()
        return from_low[y, :, :]

    def got_high(y):
        down_copy(y, own(y)).wait_recv()
        return from_high[y, :, :]

    def relay_up(y, value):
        from_low[y, :, :] = value + acc[y, cols - 1, :, :]
        up_copy(y, from_low.at[y]).start()

    def relay_down(y, value):
        from_high[y, :, :] = value + acc[y, cols - 1, :, :]
        down_copy(y, from_high.at[y]).start()

    def pass_down(y):
        down_copy(y, own(y)).wait_recv()
        down_copy(y, from_high.at[y]).start()

    def up_gone(y):
        up_copy(y, own(y)).wait_send()

    def down_gone(y):
        down_copy(y, own(y)).wait_send()

    def finish(y, before):
        def one(x, _):
            acc[y, x, :, :] = acc[y, x, :, :] + before
            return 0

        lax.fori_loop(0, cols, one, 0)

    @pl.when(lon == 0)
    def _():
        each(lambda j: up_copy(row_e(j), own(row_e(j))).start())
        each(lambda j: up_copy(row_c(j), own(row_c(j))).start())
        each(lambda j: relay_down(row_c(j), got_high(row_c(j))))
        each(lambda j: relay_down(row_e(j), got_high(row_e(j))))
        for row in (row_a, row_e, row_c):
            each(lambda j: up_gone(row(j)))
        for row in (row_b, row_c, row_e):
            each(lambda j: down_gone(row(j)))

    @pl.when(lon == 1)
    def _():
        def first(j):
            y = row_a(j)
            before = got_low(y)
            relay_up(y, before)
            relay_down(row_e(j), got_high(row_e(j)))
            finish(y, before)

        def second(j):
            y = row_e(j)
            before = got_low(y)
            relay_up(y, before)
            finish(y, before)

        def third(j):
            y = row_b(j)
            up_gone(y)
            finish(y, got_high(y))

        def fourth(j):
            y = row_c(j)
            down_gone(y)
            finish(y, got_low(y))

        for part in (first, second, third, fourth):
            each(part)
        each(lambda j: up_gone(row_a(j)))
        each(lambda j: up_gone(row_e(j)))
        each(lambda j: down_gone(row_e(j)))

    @pl.when(lon == 2)
    def _():
        def first(j):
            y = row_b(j)
            low = got_low(y)
            relay_up(y, low)
            pass_down(y)
            finish(y, low + from_high[y, :, :])

        def second(j):
            y = row_a(j)
            before = got_low(y)
            relay_up(y, before)
            finish(y, before)

        def third(j):
            y = row_c(j)
            up_gone(y)
            finish(y, got_high(y))

        def fourth(j):
            y = row_e(j)
            down_gone(y)
            finish(y, got_low(y))

        for part in (first, second, third, fourth):
            each(part)
        each(lambda j: up_gone(row_b(j)))
        each(lambda j: up_gone(row_a(j)))
        each(lambda j: down_gone(row_b(j)))

    @pl.when(lon == 3)
    def _():
        each(lambda j: pass_down(row_b(j)))
        each(lambda j: pass_down(row_c(j)))

        def both(y):
            finish(y, got_low(y) + from_high[y, :, :])

        each(lambda j: both(row_c(j)))
        each(lambda j: both(row_b(j)))
        each(lambda j: finish(row_e(j), got_high(row_e(j))))
        each(lambda j: finish(row_a(j), got_low(row_a(j))))
        each(lambda j: down_gone(row_b(j)))
        each(lambda j: down_gone(row_c(j)))


def store_kernel(acc, end, acc_out, end_out, sem):
    def both(y):
        return (
            pltpu.make_async_copy(end.at[y], end_out.at[y], sem.at[0, y]),
            pltpu.make_async_copy(acc.at[y], acc_out.at[y], sem.at[1, y]),
        )

    for y in range(acc.shape[0]):
        for copy in both(y):
            copy.start()
    for y in range(acc.shape[0]):
        for copy in both(y):
            copy.wait()


def per_device(sizes, heat, north, east, up):
    rows, cols, deep, members = heat.shape
    shape = jax.ShapeDtypeStruct(heat.shape, heat.dtype)
    f32 = jnp.float32
    dma = pltpu.SemaphoreType.DMA
    acc, end = pl.pallas_call(
        functools.partial(kernel, sizes),
        out_shape=(shape, shape),
        in_specs=[pl.BlockSpec(memory_space=pl.ANY)] * 4,
        out_specs=(pl.BlockSpec(memory_space=pltpu.VMEM),) * 2,
        scratch_shapes=[
            pltpu.VMEM((2, rows + 2, cols + 2, deep + 2 * PAD, members), f32),
            pltpu.VMEM((3, rows, cols, deep, members), f32),
            pltpu.VMEM((rows, deep, members), f32),
            pltpu.VMEM((rows, deep, members), f32),
            pltpu.VMEM((2, rows, cols, members), f32),
            pltpu.VMEM((2, rows, cols, members), f32),
            dma((4, rows)),
            dma((2, 2, rows)),
            dma((2, 2, rows)),
            dma((2, 2)),
            dma((2, 2)),
            dma((2, rows)),
            dma((2, rows)),
            dma((rows,)),
            dma((rows,)),
            dma((rows,)),
            dma((rows,)),
        ],
        compiler_params=pltpu.CompilerParams(
            collective_id=0,
            has_side_effects=True,
            vmem_limit_bytes=40 * 1024 * 1024,
        ),
    )(heat, north, east, up)
    return pl.pallas_call(
        store_kernel,
        out_shape=(shape, shape),
        in_specs=[pl.BlockSpec(memory_space=pltpu.VMEM)] * 2,
        out_specs=(pl.BlockSpec(memory_space=pltpu.HBM),) * 2,
        scratch_shapes=[dma((2, rows))],
        compiler_params=pltpu.CompilerParams(vmem_limit_bytes=1024 * 1024),
    )(acc, end)


def solution(mesh):
    sizes = tuple(mesh.shape[name] for name in ("lat", "lon", "lev"))
    spec = P("lat", "lon", "lev", None)
    return jax.shard_map(
        functools.partial(per_device, sizes),
        mesh=mesh,
        in_specs=(spec,) * 4,
        out_specs=(spec, spec),
        check_vma=False,
    )
```

```python
import functools

import jax
import jax.numpy as jnp
from jax import lax
from jax.experimental import pallas as pl
from jax.experimental.pallas import tpu as pltpu
from jax.sharding import PartitionSpec as P

STEPS = 6
PAD = 8
MESH = pl.DeviceIdType.MESH


def row_at(k, rows):
    odd = k % 2
    return (1 - odd) * (k // 2) + odd * (rows - 1 - k // 2)


def kernel(
    sizes,
    heat,
    north,
    east,
    up,
    acc,
    end,
    field,
    wind,
    from_low,
    from_high,
    edge_out,
    edge_in,
    heat_sem,
    wind_sem,
    lon_send,
    lon_recv,
    lat_send,
    lat_recv,
    lev_send,
    lev_recv,
    sum_send,
):
    lats, lons, levs = sizes
    rows, cols, deep, members = heat.shape
    lat, lon, lev = (lax.axis_index(name) for name in ("lat", "lon", "lev"))
    body = pl.ds(PAD, deep)

    def remote(src, dst, send, recv, axis, to):
        return pltpu.make_async_remote_copy(
            src_ref=src,
            dst_ref=dst,
            send_sem=send,
            recv_sem=recv,
            device_id={axis: to},
            device_id_type=MESH,
        )

    quarter, half = rows // 4, rows // 2

    def lon_copy(slot, k, side):
        y = row_at(k, rows)
        return remote(
            field.at[slot, y + 1, (1, cols)[side], body],
            field.at[slot, y + 1, (cols + 1, 0)[side], body],
            lon_send.at[side, slot, k // quarter],
            lon_recv.at[side, slot, y],
            "lon",
            lon + (-1, 1)[side],
        )

    def lon_gone(slot, part, side):
        some = field.at[slot, pl.ds(1, quarter), 1, body]
        remote(
            some,
            some,
            lon_send.at[side, slot, part],
            lon_recv.at[side, slot, 0],
            "lon",
            lon + (-1, 1)[side],
        ).wait_send()

    def lat_copy(slot, side):
        src = field.at[slot, (1, rows)[side], pl.ds(1, cols), body]
        dst = field.at[slot, (rows + 1, 0)[side], pl.ds(1, cols), body]
        to = lat + (-1, 1)[side]
        return remote(
            src, dst, lat_send.at[side, slot], lat_recv.at[side, slot], "lat", to
        )

    def lev_copy(slot, part):
        some = pl.ds(part * half, half)
        return remote(
            edge_out.at[slot, some],
            edge_in.at[slot, some],
            lev_send.at[slot, part],
            lev_recv.at[slot, part],
            "lev",
            1 - lev,
        )

    spare = STEPS % 2

    def up_copy(y, way, src):
        return remote(
            src,
            from_low.at[y],
            sum_send.at[1, way],
            lon_recv.at[1, spare, y],
            "lon",
            lon + 1,
        )

    def down_copy(y, way, src):
        return remote(
            src,
            from_high.at[y],
            sum_send.at[0, way],
            lon_recv.at[0, spare, y],
            "lon",
            (lon + lons - 1) % lons,
        )

    def sums_gone(side, way):
        some = from_low.at[pl.ds(0, quarter)]
        remote(
            some,
            some,
            sum_send.at[side, way],
            lon_recv.at[side, spare, 0],
            "lon",
            (lon + (lons - 1, 1)[side]) % lons,
        ).wait_send()

    lon_has = (lon > 0, lon < lons - 1)
    lat_has = (lat > 0, lat < lats - 1)

    def load_heat(first, count, part):
        return pltpu.make_async_copy(
            heat.at[pl.ds(first, count)],
            field.at[0, pl.ds(first + 1, count), pl.ds(1, cols), body],
            heat_sem.at[part],
        )

    def load_wind(d):
        return pltpu.make_async_copy(
            (north, east, up)[d], wind.at[d], wind_sem.at[d]
        )

    barrier = pltpu.get_barrier_semaphore()

    def greet(axis, to):
        pl.semaphore_signal(
            barrier, inc=1, device_id={axis: to}, device_id_type=MESH
        )

    for side in (0, 1):
        greet("lon", (lon + (lons - 1, 1)[side]) % lons)
        pl.when(lat_has[side])(lambda: greet("lat", lat + (-1, 1)[side]))
    greet("lev", 1 - lev)

    load_heat(0, quarter, 0).start()
    load_heat(rows - quarter, quarter, 0).start()
    load_heat(quarter, half, 1).start()

    peers = 3 + sum(has.astype(jnp.int32) for has in lat_has)
    pl.semaphore_wait(barrier, peers)

    edge_from = PAD + (1 - lev) * (deep - 1)
    edge_to = PAD - 1 + (1 - lev) * (deep + 1)

    def send_row(slot, k):
        y = row_at(k, rows)
        for side in (0, 1):
            pl.when(lon_has[side])(lambda: lon_copy(slot, k, side).start())
            pl.when(jnp.logical_and(lat_has[side], y == (0, rows - 1)[side]))(
                lambda: lat_copy(slot, side).start()
            )

    def first_row(k, _):
        send_row(0, k)
        return 0

    for part in (0, 1):
        load_heat(0, half, part).wait()
        lax.fori_loop(part * half, (part + 1) * half, first_row, 0)
    for d in range(3):
        load_wind(d).start()

    def first_edges(k, _):
        y = row_at(k, rows)

        def one(x, _):
            edge_out[0, k, pl.ds(x, 1), :] = field[
                0, y + 1, x + 1, pl.ds(edge_from, 1), :
            ]
            return 0

        lax.fori_loop(0, cols, one, 0)
        return 0

    for part in (0, 1):
        lax.fori_loop(part * half, (part + 1) * half, first_edges, 0)
        lev_copy(0, part).start()

    def clear_row(y, _):
        for slot in (0, 1):
            field[slot, y + 1, pl.ds(1, cols), pl.ds(0, PAD), :] = jnp.zeros(
                (cols, PAD, members), jnp.float32
            )
            field[slot, y + 1, pl.ds(1, cols), pl.ds(PAD + deep, PAD), :] = jnp.zeros(
                (cols, PAD, members), jnp.float32
            )
            for side in (0, 1):

                @pl.when(jnp.logical_not(lon_has[side]))
                def _():
                    field[slot, y + 1, (0, cols + 1)[side], body, :] = jnp.zeros(
                        (deep, members), jnp.float32
                    )

        return 0

    lax.fori_loop(0, rows, clear_row, 0)

    def clear_lat(x, _):
        for slot in (0, 1):
            for side in (0, 1):

                @pl.when(jnp.logical_not(lat_has[side]))
                def _():
                    field[slot, (0, rows + 1)[side], x + 1, body, :] = jnp.zeros(
                        (deep, members), jnp.float32
                    )

        return 0

    lax.fori_loop(0, cols, clear_lat, 0)

    def updated(slot, k, y, x):
        field[slot, y + 1, x + 1, pl.ds(edge_to, 1), :] = edge_in[
            slot, k, pl.ds(x, 1), :
        ]
        middle = field[slot, y + 1, x + 1, body, :]
        lower = (
            field[slot, y, x + 1, body, :],
            field[slot, y + 1, x, body, :],
            field[slot, y + 1, x + 1, pl.ds(PAD - 1, deep), :],
        )
        upper = (
            field[slot, y + 2, x + 1, body, :],
            field[slot, y + 1, x + 2, body, :],
            field[slot, y + 1, x + 1, pl.ds(PAD + 1, deep), :],
        )
        spread = (
            lower[0] + upper[0] + lower[1] + upper[1] + lower[2] + upper[2]
        ) - 6.0 * middle
        value = middle + 0.05 * spread
        for d in range(3):
            value = value - wind[d, y, x, :, :] * (upper[d] - lower[d])
        return value

    def arrivals(slot, k):
        y = row_at(k, rows)
        for side in (0, 1):
            pl.when(lon_has[side])(lambda: lon_copy(slot, k, 1 - side).wait_recv())
            pl.when(jnp.logical_and(lat_has[side], y == (0, rows - 1)[side]))(
                lambda: lat_copy(slot, 1 - side).wait_recv()
            )
        pl.when(k % half == 0)(lambda: lev_copy(slot, k // half).wait_recv())

    def departures(slot, k):
        y = row_at(k, rows)
        for side in (0, 1):
            pl.when(jnp.logical_and(lon_has[side], k % quarter == 0))(
                lambda: lon_gone(slot, k // quarter, side)
            )
            pl.when(jnp.logical_and(lat_has[side], y == (0, rows - 1)[side]))(
                lambda: lat_copy(slot, side).wait_send()
            )
        pl.when(k % half == 0)(lambda: lev_copy(slot, k // half).wait_send())

    def step(t, _):
        now = t % 2
        later = 1 - now

        @pl.when(t == 0)
        def _():
            for d in range(3):
                load_wind(d).wait()

        def one_row(k, _):
            y = row_at(k, rows)
            arrivals(now, k)
            pl.when(t > 0)(lambda: departures(later, k))

            def one(x, _):
                field[later, y + 1, x + 1, body, :] = updated(now, k, y, x)
                edge_out[later, k, pl.ds(x, 1), :] = field[
                    later, y + 1, x + 1, pl.ds(edge_from, 1), :
                ]
                return 0

            lax.fori_loop(0, cols, one, 0)
            send_row(later, k)
            pl.when(k % half == half - 1)(lambda: lev_copy(later, k // half).start())
            return 0

        lax.fori_loop(0, rows, one_row, 0)
        return 0

    lax.fori_loop(0, STEPS - 1, step, 0)

    last = (STEPS - 1) % 2
    scale = 1.0 / (cols * lons)

    way_b, way_e, way_a, way_c = range(4)

    def row_b(j):
        return row_at(4 * j, rows)

    def row_e(j):
        return row_at(4 * j + 1, rows)

    def row_a(j):
        return row_at(4 * j + 2, rows)

    def row_c(j):
        return row_at(4 * j + 3, rows)

    def own(y):
        return acc.at[y, cols - 1]

    def each(body_of):
        def one(j, _):
            body_of(j)
            return 0

        lax.fori_loop(0, quarter, one, 0)

    def last_row(k, _):
        y = row_at(k, rows)
        way = k % 4
        arrivals(last, k)
        departures(spare, k)

        def one(x, total):
            value = updated(last, k, y, x)
            end[y, x, :, :] = value
            total = total + value
            acc[y, x, :, :] = total * scale
            return total

        lax.fori_loop(0, cols, one, jnp.zeros((deep, members), jnp.float32))

        def first(place, number):
            return jnp.logical_and(lon == place, way == number)

        up_first = jnp.logical_or(
            first(0, 2), jnp.logical_or(first(1, 0), first(2, 3))
        )
        down_first = jnp.logical_or(
            first(0, 0), jnp.logical_or(first(1, 3), first(2, 1))
        )
        pl.when(up_first)(lambda: up_copy(y, way, own(y)).start())
        pl.when(down_first)(lambda: down_copy(y, way, own(y)).start())
        return 0

    lax.fori_loop(0, rows, last_row, 0)

    def halo_gone(k, _):
        departures(last, k)
        return 0

    lax.fori_loop(0, rows, halo_gone, 0)

    def got_low(y):
        up_copy(y, 0, own(y)).wait_recv()
        return from_low[y, :, :]

    def got_high(y):
        down_copy(y, 0, own(y)).wait_recv()
        return from_high[y, :, :]

    def relay_up(y, way, value):
        from_low[y, :, :] = value + acc[y, cols - 1, :, :]
        up_copy(y, way, from_low.at[y]).start()

    def relay_down(y, way, value):
        from_high[y, :, :] = value + acc[y, cols - 1, :, :]
        down_copy(y, way, from_high.at[y]).start()

    def pass_down(y, way):
        down_copy(y, 0, own(y)).wait_recv()
        down_copy(y, way, from_high.at[y]).start()

    def finish(y, before):
        def one(x, _):
            acc[y, x, :, :] = acc[y, x, :, :] + before
            return 0

        lax.fori_loop(0, cols, one, 0)

    def drain(up, down):
        for way in up:
            sums_gone(1, way)
        for way in down:
            sums_gone(0, way)

    @pl.when(lon == 0)
    def _():
        each(lambda j: up_copy(row_e(j), way_e, own(row_e(j))).start())
        each(lambda j: up_copy(row_c(j), way_c, own(row_c(j))).start())
        each(lambda j: relay_down(row_c(j), way_c, got_high(row_c(j))))
        each(lambda j: relay_down(row_e(j), way_e, got_high(row_e(j))))
        drain((way_a, way_e, way_c), (way_b, way_c, way_e))

    @pl.when(lon == 1)
    def _():
        def first(j):
            y = row_a(j)
            before = got_low(y)
            relay_up(y, way_a, before)
            relay_down(row_e(j), way_e, got_high(row_e(j)))
            finish(y, before)

        def second(j):
            y = row_e(j)
            before = got_low(y)
            relay_up(y, way_e, before)
            finish(y, before)

        each(first)
        each(second)
        drain((way_b,), (way_c,))
        each(lambda j: finish(row_b(j), got_high(row_b(j))))
        each(lambda j: finish(row_c(j), got_low(row_c(j))))
        drain((way_a, way_e), (way_e,))

    @pl.when(lon == 2)
    def _():
        def first(j):
            y = row_b(j)
            low = got_low(y)
            relay_up(y, way_b, low)
            pass_down(y, way_b)
            finish(y, low + from_high[y, :, :])

        def second(j):
            y = row_a(j)
            before = got_low(y)
            relay_up(y, way_a, before)
            finish(y, before)

        each(first)
        each(second)
        drain((way_c,), (way_e,))
        each(lambda j: finish(row_c(j), got_high(row_c(j))))
        each(lambda j: finish(row_e(j), got_low(row_e(j))))
        drain((way_b, way_a), (way_b,))

    @pl.when(lon == 3)
    def _():
        each(lambda j: pass_down(row_b(j), way_b))
        each(lambda j: pass_down(row_c(j), way_c))

        def both(y):
            finish(y, got_low(y) + from_high[y, :, :])

        each(lambda j: both(row_c(j)))
        each(lambda j: both(row_b(j)))
        each(lambda j: finish(row_e(j), got_high(row_e(j))))
        each(lambda j: finish(row_a(j), got_low(row_a(j))))
        drain((), (way_b, way_c))


def store_kernel(acc, end, acc_out, end_out, sem):
    pairs = ((end, end_out), (acc, acc_out))
    for y in range(acc.shape[0]):
        for i, (src, dst) in enumerate(pairs):
            pltpu.make_async_copy(src.at[y], dst.at[y], sem.at[i]).start()
    for i, (src, dst) in enumerate(pairs):
        pltpu.make_async_copy(src, dst, sem.at[i]).wait()


def per_device(sizes, heat, north, east, up):
    rows, cols, deep, members = heat.shape
    shape = jax.ShapeDtypeStruct(heat.shape, heat.dtype)
    f32 = jnp.float32
    dma = pltpu.SemaphoreType.DMA
    acc, end = pl.pallas_call(
        functools.partial(kernel, sizes),
        out_shape=(shape, shape),
        in_specs=[pl.BlockSpec(memory_space=pl.ANY)] * 4,
        out_specs=(pl.BlockSpec(memory_space=pltpu.VMEM),) * 2,
        scratch_shapes=[
            pltpu.VMEM((2, rows + 2, cols + 2, deep + 2 * PAD, members), f32),
            pltpu.VMEM((3, rows, cols, deep, members), f32),
            pltpu.VMEM((rows, deep, members), f32),
            pltpu.VMEM((rows, deep, members), f32),
            pltpu.VMEM((2, rows, cols, members), f32),
            pltpu.VMEM((2, rows, cols, members), f32),
            dma((2,)),
            dma((3,)),
            dma((2, 2, 4)),
            dma((2, 2, rows)),
            dma((2, 2)),
            dma((2, 2)),
            dma((2, 2)),
            dma((2, 2)),
            dma((2, 4)),
        ],
        compiler_params=pltpu.CompilerParams(
            collective_id=0,
            has_side_effects=True,
            vmem_limit_bytes=40 * 1024 * 1024,
        ),
    )(heat, north, east, up)
    return pl.pallas_call(
        store_kernel,
        out_shape=(shape, shape),
        in_specs=[pl.BlockSpec(memory_space=pltpu.VMEM)] * 2,
        out_specs=(pl.BlockSpec(memory_space=pltpu.HBM),) * 2,
        scratch_shapes=[dma((2,))],
        compiler_params=pltpu.CompilerParams(vmem_limit_bytes=1024 * 1024),
    )(acc, end)


def solution(mesh):
    sizes = tuple(mesh.shape[name] for name in ("lat", "lon", "lev"))
    spec = P("lat", "lon", "lev", None)
    return jax.shard_map(
        functools.partial(per_device, sizes),
        mesh=mesh,
        in_specs=(spec,) * 4,
        out_specs=(spec, spec),
        check_vma=False,
    )
```

```python
import functools

import jax
import jax.numpy as jnp
from jax import lax
from jax.experimental import pallas as pl
from jax.experimental.pallas import tpu as pltpu
from jax.sharding import PartitionSpec as P

STEPS = 6
PAD = 8
MESH = pl.DeviceIdType.MESH


def row_at(k, rows):
    odd = k % 2
    return (1 - odd) * (k // 2) + odd * (rows - 1 - k // 2)


def kernel(
    sizes,
    heat,
    north,
    east,
    up,
    acc,
    end,
    field,
    wind,
    from_low,
    from_high,
    edge_out,
    edge_in,
    heat_sem,
    wind_sem,
    lon_send,
    lon_recv,
    lat_send,
    lat_recv,
    lev_send,
    lev_recv,
    sum_send,
    sum_recv,
):
    lats, lons, levs = sizes
    rows, cols, deep, members = heat.shape
    lat, lon, lev = (lax.axis_index(name) for name in ("lat", "lon", "lev"))
    body = pl.ds(PAD, deep)

    def remote(src, dst, send, recv, axis, to):
        return pltpu.make_async_remote_copy(
            src_ref=src,
            dst_ref=dst,
            send_sem=send,
            recv_sem=recv,
            device_id={axis: to},
            device_id_type=MESH,
        )

    quarter, half = rows // 4, rows // 2

    def lon_copy(slot, k, side):
        y = row_at(k, rows)
        return remote(
            field.at[slot, y + 1, (1, cols)[side], body],
            field.at[slot, y + 1, (cols + 1, 0)[side], body],
            lon_send.at[side, slot, k // half],
            lon_recv.at[slot, y],
            "lon",
            (lon + (lons - 1, 1)[side]) % lons,
        )

    def lon_gone(slot, part, side):
        some = field.at[slot, pl.ds(1, half), 1, body]
        remote(
            some,
            some,
            lon_send.at[side, slot, part],
            lon_recv.at[slot, 0],
            "lon",
            (lon + (lons - 1, 1)[side]) % lons,
        ).wait_send()

    def lon_here(slot, y, count):
        some = field.at[slot, pl.ds(1, count), 1, body]
        remote(
            some,
            some,
            lon_send.at[0, slot, 0],
            lon_recv.at[slot, y],
            "lon",
            (lon + 1) % lons,
        ).wait_recv()

    def lat_copy(slot, side):
        src = field.at[slot, (1, rows)[side], pl.ds(1, cols), body]
        dst = field.at[slot, (rows + 1, 0)[side], pl.ds(1, cols), body]
        to = (lat + (lats - 1, 1)[side]) % lats
        return remote(
            src, dst, lat_send.at[side, slot], lat_recv.at[side, slot], "lat", to
        )

    def lev_copy(slot, part):
        some = pl.ds(part * half, half)
        return remote(
            edge_out.at[slot, some],
            edge_in.at[slot, some],
            lev_send.at[slot, part],
            lev_recv.at[slot, part],
            "lev",
            1 - lev,
        )

    own_sums, relayed = 0, 1
    spare = STEPS % 2

    def up_copy(y, kind, src):
        return remote(
            src,
            from_low.at[y],
            sum_send.at[kind],
            lon_recv.at[spare, y],
            "lon",
            (lon + 1) % lons,
        )

    def down_copy(y, kind, src):
        return remote(
            src,
            from_high.at[y],
            sum_send.at[kind],
            sum_recv.at[y],
            "lon",
            (lon + lons - 1) % lons,
        )

    def sums_gone(kind, count):
        some = from_low.at[pl.ds(0, count)]
        remote(
            some, some, sum_send.at[kind], sum_recv.at[0], "lon", (lon + 1) % lons
        ).wait_send()

    lon_has = (lon > 0, lon < lons - 1)
    lat_has = (lat > 0, lat < lats - 1)

    def load_heat(first, count, part):
        return pltpu.make_async_copy(
            heat.at[pl.ds(first, count)],
            field.at[0, pl.ds(first + 1, count), pl.ds(1, cols), body],
            heat_sem.at[part],
        )

    def load_wind(d):
        return pltpu.make_async_copy(
            (north, east, up)[d], wind.at[d], wind_sem.at[d]
        )

    barrier = pltpu.get_barrier_semaphore()

    def greet(axis, to):
        pl.semaphore_signal(
            barrier, inc=1, device_id={axis: to}, device_id_type=MESH
        )

    for side in (0, 1):
        greet("lon", (lon + (lons - 1, 1)[side]) % lons)
        pl.when(lat_has[side])(lambda: greet("lat", lat + (-1, 1)[side]))
    greet("lev", 1 - lev)

    load_heat(0, quarter, 0).start()
    load_heat(rows - quarter, quarter, 0).start()
    load_heat(quarter, half, 1).start()

    peers = 3 + sum(has.astype(jnp.int32) for has in lat_has)
    pl.semaphore_wait(barrier, peers)

    edge_from = PAD + (1 - lev) * (deep - 1)
    edge_to = PAD - 1 + (1 - lev) * (deep + 1)

    def send_row(slot, k):
        y = row_at(k, rows)
        for side in (0, 1):
            pl.when(lon_has[side])(lambda: lon_copy(slot, k, side).start())
            pl.when(jnp.logical_and(lat_has[side], y == (0, rows - 1)[side]))(
                lambda: lat_copy(slot, side).start()
            )

    def first_row(k, _):
        send_row(0, k)
        return 0

    for part in (0, 1):
        load_heat(0, half, part).wait()
        lax.fori_loop(part * half, (part + 1) * half, first_row, 0)
    for d in range(3):
        load_wind(d).start()

    def first_edges(k, _):
        y = row_at(k, rows)

        def one(x, _):
            edge_out[0, k, pl.ds(x, 1), :] = field[
                0, y + 1, x + 1, pl.ds(edge_from, 1), :
            ]
            return 0

        lax.fori_loop(0, cols, one, 0)
        return 0

    for part in (0, 1):
        lax.fori_loop(part * half, (part + 1) * half, first_edges, 0)
        lev_copy(0, part).start()

    def clear_row(y, _):
        for slot in (0, 1):
            field[slot, y + 1, pl.ds(1, cols), pl.ds(0, PAD), :] = jnp.zeros(
                (cols, PAD, members), jnp.float32
            )
            field[slot, y + 1, pl.ds(1, cols), pl.ds(PAD + deep, PAD), :] = jnp.zeros(
                (cols, PAD, members), jnp.float32
            )
            for side in (0, 1):

                @pl.when(jnp.logical_not(lon_has[side]))
                def _():
                    field[slot, y + 1, (0, cols + 1)[side], body, :] = jnp.zeros(
                        (deep, members), jnp.float32
                    )

        return 0

    lax.fori_loop(0, rows, clear_row, 0)

    def clear_lat(x, _):
        for slot in (0, 1):
            for side in (0, 1):

                @pl.when(jnp.logical_not(lat_has[side]))
                def _():
                    field[slot, (0, rows + 1)[side], x + 1, body, :] = jnp.zeros(
                        (deep, members), jnp.float32
                    )

        return 0

    lax.fori_loop(0, cols, clear_lat, 0)

    def updated(slot, k, y, x):
        field[slot, y + 1, x + 1, pl.ds(edge_to, 1), :] = edge_in[
            slot, k, pl.ds(x, 1), :
        ]
        middle = field[slot, y + 1, x + 1, body, :]
        lower = (
            field[slot, y, x + 1, body, :],
            field[slot, y + 1, x, body, :],
            field[slot, y + 1, x + 1, pl.ds(PAD - 1, deep), :],
        )
        upper = (
            field[slot, y + 2, x + 1, body, :],
            field[slot, y + 1, x + 2, body, :],
            field[slot, y + 1, x + 1, pl.ds(PAD + 1, deep), :],
        )
        spread = (
            lower[0] + upper[0] + lower[1] + upper[1] + lower[2] + upper[2]
        ) - 6.0 * middle
        value = middle + 0.05 * spread
        for d in range(3):
            value = value - wind[d, y, x, :, :] * (upper[d] - lower[d])
        return value

    def arrivals(slot, k):
        y = row_at(k, rows)
        both = jnp.logical_and(*lon_has)
        pl.when(both)(lambda: lon_here(slot, y, 2))
        pl.when(jnp.logical_not(both))(lambda: lon_here(slot, y, 1))
        for side in (0, 1):
            pl.when(jnp.logical_and(lat_has[side], y == (0, rows - 1)[side]))(
                lambda: lat_copy(slot, 1 - side).wait_recv()
            )
        pl.when(k % half == 0)(lambda: lev_copy(slot, k // half).wait_recv())

    def departures(slot, k):
        y = row_at(k, rows)
        for side in (0, 1):
            pl.when(jnp.logical_and(lon_has[side], k % half == 0))(
                lambda: lon_gone(slot, k // half, side)
            )
            pl.when(jnp.logical_and(lat_has[side], y == (0, rows - 1)[side]))(
                lambda: lat_copy(slot, side).wait_send()
            )
        pl.when(k % half == 0)(lambda: lev_copy(slot, k // half).wait_send())

    def step(t, _):
        now = t % 2
        later = 1 - now

        @pl.when(t == 0)
        def _():
            for d in range(3):
                load_wind(d).wait()

        def one_row(k, _):
            y = row_at(k, rows)
            arrivals(now, k)
            pl.when(t > 0)(lambda: departures(later, k))

            def one(x, _):
                field[later, y + 1, x + 1, body, :] = updated(now, k, y, x)
                edge_out[later, k, pl.ds(x, 1), :] = field[
                    later, y + 1, x + 1, pl.ds(edge_from, 1), :
                ]
                return 0

            lax.fori_loop(0, cols, one, 0)
            send_row(later, k)
            pl.when(k % half == half - 1)(lambda: lev_copy(later, k // half).start())
            return 0

        lax.fori_loop(0, rows, one_row, 0)
        return 0

    lax.fori_loop(0, STEPS - 1, step, 0)

    last = (STEPS - 1) % 2
    scale = 1.0 / (cols * lons)

    def row_b(j):
        return row_at(4 * j, rows)

    def row_e(j):
        return row_at(4 * j + 1, rows)

    def row_a(j):
        return row_at(4 * j + 2, rows)

    def row_c(j):
        return row_at(4 * j + 3, rows)

    def own(y):
        return acc.at[y, cols - 1]

    def each(body_of):
        def one(j, _):
            body_of(j)
            return 0

        lax.fori_loop(0, quarter, one, 0)

    def last_row(k, _):
        y = row_at(k, rows)
        way = k % 4
        arrivals(last, k)
        departures(spare, k)

        def one(x, total):
            value = updated(last, k, y, x)
            end[y, x, :, :] = value
            total = total + value
            acc[y, x, :, :] = total * scale
            return total

        lax.fori_loop(0, cols, one, jnp.zeros((deep, members), jnp.float32))

        def first(place, number):
            return jnp.logical_and(lon == place, way == number)

        up_first = jnp.logical_or(
            first(0, 2), jnp.logical_or(first(1, 0), first(2, 3))
        )
        down_first = jnp.logical_or(
            first(0, 0), jnp.logical_or(first(1, 3), first(2, 1))
        )
        pl.when(up_first)(lambda: up_copy(y, own_sums, own(y)).start())
        pl.when(down_first)(lambda: down_copy(y, own_sums, own(y)).start())
        return 0

    lax.fori_loop(0, rows, last_row, 0)

    def halo_gone(k, _):
        departures(last, k)
        return 0

    lax.fori_loop(0, rows, halo_gone, 0)

    def got_low(y):
        up_copy(y, 0, own(y)).wait_recv()
        return from_low[y, :, :]

    def got_high(y):
        down_copy(y, 0, own(y)).wait_recv()
        return from_high[y, :, :]

    def relay_up(y, value):
        from_low[y, :, :] = value + acc[y, cols - 1, :, :]
        up_copy(y, relayed, from_low.at[y]).start()

    def relay_down(y, value):
        from_high[y, :, :] = value + acc[y, cols - 1, :, :]
        down_copy(y, relayed, from_high.at[y]).start()

    def pass_down(y):
        down_copy(y, 0, own(y)).wait_recv()
        down_copy(y, relayed, from_high.at[y]).start()

    def finish(y, before):
        def one(x, _):
            acc[y, x, :, :] = acc[y, x, :, :] + before
            return 0

        lax.fori_loop(0, cols, one, 0)

    @pl.when(lon == 0)
    def _():
        each(lambda j: up_copy(row_e(j), own_sums, own(row_e(j))).start())
        each(lambda j: up_copy(row_c(j), own_sums, own(row_c(j))).start())
        each(lambda j: relay_down(row_c(j), got_high(row_c(j))))
        each(lambda j: relay_down(row_e(j), got_high(row_e(j))))
        sums_gone(own_sums, 4 * quarter)
        sums_gone(relayed, 2 * quarter)

    @pl.when(lon == 1)
    def _():
        def first(j):
            y = row_a(j)
            before = got_low(y)
            relay_up(y, before)
            relay_down(row_e(j), got_high(row_e(j)))
            finish(y, before)

        def second(j):
            y = row_e(j)
            before = got_low(y)
            relay_up(y, before)
            finish(y, before)

        each(first)
        each(second)
        sums_gone(own_sums, 2 * quarter)
        each(lambda j: finish(row_b(j), got_high(row_b(j))))
        each(lambda j: finish(row_c(j), got_low(row_c(j))))
        sums_gone(relayed, 3 * quarter)

    @pl.when(lon == 2)
    def _():
        def first(j):
            y = row_b(j)
            low = got_low(y)
            relay_up(y, low)
            pass_down(y)
            finish(y, low + from_high[y, :, :])

        def second(j):
            y = row_a(j)
            before = got_low(y)
            relay_up(y, before)
            finish(y, before)

        each(first)
        each(second)
        sums_gone(own_sums, 2 * quarter)
        each(lambda j: finish(row_c(j), got_high(row_c(j))))
        each(lambda j: finish(row_e(j), got_low(row_e(j))))
        sums_gone(relayed, 3 * quarter)

    @pl.when(lon == 3)
    def _():
        each(lambda j: pass_down(row_b(j)))
        each(lambda j: pass_down(row_c(j)))

        def both(y):
            finish(y, got_low(y) + from_high[y, :, :])

        each(lambda j: both(row_c(j)))
        each(lambda j: both(row_b(j)))
        each(lambda j: finish(row_e(j), got_high(row_e(j))))
        each(lambda j: finish(row_a(j), got_low(row_a(j))))
        sums_gone(relayed, 2 * quarter)


def store_kernel(acc, end, acc_out, end_out, sem):
    pairs = ((end, end_out), (acc, acc_out))
    for y in range(acc.shape[0]):
        for i, (src, dst) in enumerate(pairs):
            pltpu.make_async_copy(src.at[y], dst.at[y], sem.at[i]).start()
    for i, (src, dst) in enumerate(pairs):
        pltpu.make_async_copy(src, dst, sem.at[i]).wait()


def per_device(sizes, heat, north, east, up):
    rows, cols, deep, members = heat.shape
    shape = jax.ShapeDtypeStruct(heat.shape, heat.dtype)
    f32 = jnp.float32
    dma = pltpu.SemaphoreType.DMA
    acc, end = pl.pallas_call(
        functools.partial(kernel, sizes),
        out_shape=(shape, shape),
        in_specs=[pl.BlockSpec(memory_space=pl.ANY)] * 4,
        out_specs=(pl.BlockSpec(memory_space=pltpu.VMEM),) * 2,
        scratch_shapes=[
            pltpu.VMEM((2, rows + 2, cols + 2, deep + 2 * PAD, members), f32),
            pltpu.VMEM((3, rows, cols, deep, members), f32),
            pltpu.VMEM((rows, deep, members), f32),
            pltpu.VMEM((rows, deep, members), f32),
            pltpu.VMEM((2, rows, cols, members), f32),
            pltpu.VMEM((2, rows, cols, members), f32),
            dma((2,)),
            dma((3,)),
            dma((2, 2, 2)),
            dma((2, rows)),
            dma((2, 2)),
            dma((2, 2)),
            dma((2, 2)),
            dma((2, 2)),
            dma((2,)),
            dma((rows,)),
        ],
        compiler_params=pltpu.CompilerParams(
            collective_id=0,
            has_side_effects=True,
            vmem_limit_bytes=40 * 1024 * 1024,
        ),
    )(heat, north, east, up)
    return pl.pallas_call(
        store_kernel,
        out_shape=(shape, shape),
        in_specs=[pl.BlockSpec(memory_space=pltpu.VMEM)] * 2,
        out_specs=(pl.BlockSpec(memory_space=pltpu.HBM),) * 2,
        scratch_shapes=[dma((2,))],
        compiler_params=pltpu.CompilerParams(vmem_limit_bytes=1024 * 1024),
    )(acc, end)


def solution(mesh):
    sizes = tuple(mesh.shape[name] for name in ("lat", "lon", "lev"))
    spec = P("lat", "lon", "lev", None)
    return jax.shard_map(
        functools.partial(per_device, sizes),
        mesh=mesh,
        in_specs=(spec,) * 4,
        out_specs=(spec, spec),
        check_vma=False,
    )
```
